128 devices in a mesh: section: 8 (over y, core), tp: 16 (over x, z).
Axes of the slice: x: 4, y: 4, z: 4, core: 2. Of those that a mesh axis runs over, the one named last changes fastest.
Arguments:
- token_ids: int32 [2, 128], replicated, may hold values from 0 to 65535
- alpha_num: int32 [1], replicated, may hold values from 3 to 7
- embed_table: bfloat16 [65536, 8192], P('section', 'tp'), may hold values from -6 to 6
- norm_gain: float32 [8, 8192], P('section'), may hold values from 0.5 to 1.5
- w_query: bfloat16 [8, 8192, 4096], P('section', None, 'tp'), may hold values from -4 to 4
- w_key: bfloat16 [8, 8192, 512], P('section', None, 'tp'), may hold values from -4 to 4
- w_value: bfloat16 [8, 8192, 512], P('section', None, 'tp'), may hold values from -0.0625 to 0.0625
- w_out: bfloat16 [8, 4096, 8192], P('section', 'tp'), may hold values from -0.09375 to 0.09375
Outputs:
- layer_out: bfloat16 [8, 2, 128, 8192], P('section', None, 'tp')
- scales_in: float32 [8, 8192], P('section')
- scales_out: float32 [8, 4096], P('section', 'tp')
- smoothed_q: bfloat16 [8, 8192, 4096], P('section', None, 'tp')
- smoothed_k: bfloat16 [8, 8192, 512], P('section', None, 'tp')
- smoothed_v: bfloat16 [8, 8192, 512], P('section', None, 'tp')
The draws below stay inside these ranges and needn't reach their ends.
All inputs are finite; a program needn't handle non-finite values.
Results may differ from the reference program's by a relative error of at most 0.028.
Values may be sent and summed in bfloat16 or wider, within the bound.
No kernel may reach another device: no remote copies, remote signals or barrier semaphores. Data moves between devices by JAX's collectives and lax.ppermute only.
A program may use at most 128 MiB of HBM per device.

```python
import math
import jax
import jax.numpy as jnp
import numpy as np
from jax import lax

D = 8192
HEADS = 32
KV_HEADS = 4
HEAD_DIM = 128
VOCAB = 65536
SEQ = 128
MICRO = 2
LAYERS = 8
QD = 4096
KVD = 512
N_TP = 16


def draw_w_key(key, part):
    fresh = jax.random.normal(jax.random.fold_in(key, 23), (LAYERS, D, KV_HEADS * HEAD_DIM), jnp.float32)
    return (fresh / math.sqrt(D)).astype(jnp.bfloat16)


def draw_w_query(key, part):
    noise = jax.random.normal(jax.random.fold_in(key, 29), (LAYERS, D, HEADS * HEAD_DIM), jnp.float32) / math.sqrt(D)
    return noise.astype(jnp.bfloat16)


def plant(drawn, rng, least, largest):
    place = [jax.random.randint(jax.random.fold_in(rng, axis), (), 0, length) for axis, length in enumerate(drawn.shape)]
    main_axis = drawn.shape.index(max(drawn.shape))
    next_to = place[:main_axis] + [(place[main_axis] + 1) % drawn.shape[main_axis]] + place[main_axis + 1:]
    return drawn.at[tuple(place)].set(least).at[tuple(next_to)].set(largest)


def shard_levels(rng, shape, split, smallest, largest):
    def one(dim, blocks):
        heights = jax.random.uniform(jax.random.fold_in(jax.random.fold_in(rng, 6), dim), (blocks,), jnp.float32, smallest / len(split), largest / len(split))
        return jnp.repeat(jnp.exp(heights), shape[dim] // blocks).reshape((-1,) + (1,) * (len(shape) - dim - 1))

    gain = one(*split[0])
    for cut in split[1:]:
        gain = gain * one(*cut)
    return gain


def rank_table(amount, slope):
    portions = [(1 << 20) // math.isqrt(standing ** slope) + 1 for standing in range(1, amount + 1)]
    width = 1 + sum(portions) // (1 << 30)
    return np.cumsum(np.array([max(1, weight // width) for weight in portions]))


def ranked(rng, extent, count, skew):
    listing = rank_table(count, skew)
    lot = jax.random.randint(jax.random.fold_in(rng, 1), extent, 0, int(listing[count - 1]))
    rank = jnp.searchsorted(jnp.asarray(listing, jnp.int32), lot, side="right")
    return jax.random.permutation(jax.random.fold_in(rng, 2), count)[rank].astype(jnp.int32)


def centred(rng, shape, width, limit, split=(), held_as=jnp.bfloat16):
    result = jax.random.normal(rng, shape, jnp.float32) * width
    if len(split) > 0:
        result = shard_levels(rng, shape, split, -0.22, 0.18) * result
    return jnp.clip(result, min=-limit, max=limit).astype(held_as)


def setup_inputs(seed: int = 0) -> dict:
    keys = jax.random.split(jax.random.key(seed), 9)
    return {
        "token_ids": plant(ranked(keys[0], (MICRO, SEQ), VOCAB, 2), jax.random.fold_in(keys[0], 3), 0, VOCAB - 1).astype(jnp.int32),
        "alpha_num": jax.random.randint(keys[1], (1,), 3, 8).astype(jnp.int32),
        "embed_table": centred(keys[2], (VOCAB, D), 1.0, 6.0, ((0, 8), (1, 16))),
        "norm_gain": jnp.clip(1.0 + 0.1 * jax.random.normal(keys[3], (LAYERS, D), jnp.float32), 0.5, 1.5),
        "w_query": draw_w_query(jax.random.fold_in(keys[8], 71), 0),
        "w_key": draw_w_key(jax.random.fold_in(keys[8], 71), 0),
        "w_value": centred(keys[6], (LAYERS, D, KVD), D ** -0.5, 0.0625, ((0, 8), (2, 16))),
        "w_out": centred(keys[7], (LAYERS, QD, D), QD ** -0.5, 0.09375, ((0, 8), (1, 16))),
    }


norm_eps = 1e-05
stat_eps = 1e-05
rope_base = 500000.0

def rope_tables(length, head_size):
    halves = head_size // 2
    freqs = jnp.exp(-math.log(rope_base) * 2.0 * jnp.arange(halves, dtype=jnp.float32) / head_size)
    angles = jnp.arange(length, dtype=jnp.float32)[:, None] * freqs[None, :]
    return (jnp.cos(angles), jnp.sin(angles))

def rotate(values, cosine, sine):
    halves = values.shape[-1] // 2
    lower = values[..., :halves]
    upper = values[..., halves:]
    cos_rows = cosine[:, None, :]
    sin_rows = sine[:, None, :]
    return jnp.concatenate([lower * cos_rows - upper * sin_rows, upper * cos_rows + lower * sin_rows], axis=-1)

def smoothing(act_peak, weight_peak, alpha_exp):
    return jnp.exp(alpha_exp * jnp.log(act_peak + stat_eps) - (1.0 - alpha_exp) * jnp.log(weight_peak + stat_eps))

def attention_layer(resid, gain_row, query_w, key_w, value_w, out_w):
    length = resid.shape[0]
    values = resid.astype(jnp.float32)
    square = lax.optimization_barrier(jnp.mean(values * values, axis=1, keepdims=True))
    normed = (values * lax.rsqrt(square + norm_eps) * gain_row[None, :]).astype(jnp.bfloat16)
    query = jnp.dot(normed, query_w, preferred_element_type=jnp.float32)
    key_rows = lax.optimization_barrier(jnp.dot(normed, key_w, preferred_element_type=jnp.float32).astype(jnp.bfloat16))
    value_rows = jnp.dot(normed, value_w, preferred_element_type=jnp.float32).astype(jnp.bfloat16)
    cosine, sine = rope_tables(length, HEAD_DIM)
    query_rot = rotate(query.reshape(length, HEADS, HEAD_DIM), cosine, sine).astype(jnp.bfloat16)
    key_rot = rotate(key_rows.astype(jnp.float32).reshape(length, KV_HEADS, HEAD_DIM), cosine, sine).astype(jnp.bfloat16)
    group_size = HEADS // KV_HEADS
    grouped = query_rot.reshape(length, group_size, KV_HEADS, HEAD_DIM).astype(jnp.float32)
    scores = jnp.einsum('qrgd,kgd->grqk', grouped, key_rot.astype(jnp.float32)) / math.sqrt(HEAD_DIM)
    positions = jnp.arange(length, dtype=jnp.int32)
    causal = positions[:, None] >= positions[None, :]
    scores = jnp.where(causal[None, None], scores, -1e+30)
    probs = jax.nn.softmax(scores, axis=-1).astype(jnp.bfloat16)
    value_heads = value_rows.reshape(length, KV_HEADS, HEAD_DIM).astype(jnp.float32)
    attended = jnp.einsum('grqk,kgd->qrgd', probs.astype(jnp.float32), value_heads)
    attended = attended.reshape(length, HEADS * HEAD_DIM).astype(jnp.bfloat16)
    group_cols = HEADS * HEAD_DIM // N_TP
    head_parts = jnp.einsum('qnc,ncd->nqd', attended.reshape(length, N_TP, group_cols).astype(jnp.float32), out_w.reshape(N_TP, group_cols, D).astype(jnp.float32)).astype(jnp.bfloat16)
    mixed = lax.optimization_barrier(jnp.sum(head_parts.astype(jnp.float32), axis=0))
    output = lax.optimization_barrier((values + mixed).astype(jnp.bfloat16))
    normed_peak = lax.optimization_barrier(jnp.max(jnp.abs(normed), axis=0)).astype(jnp.float32)
    attended_peak = lax.optimization_barrier(jnp.max(jnp.abs(attended), axis=0)).astype(jnp.float32)
    return (output, normed_peak, attended_peak)

def reference(token_ids, alpha_num, embed_table, norm_gain, w_query, w_key, w_value, w_out):
    alpha_exp = alpha_num[0].astype(jnp.float32) / 10.0
    stream = jnp.take(embed_table, token_ids, axis=0)
    outputs = []
    inputs_scales = []
    output_scales = []
    smooth_query = []
    smooth_key = []
    smooth_value = []
    for layer_index in range(LAYERS):

        def advance(carry, resid):
            act_peak, head_peak = carry
            output, normed_peak, attended_peak = attention_layer(resid, norm_gain[layer_index], w_query[layer_index], w_key[layer_index], w_value[layer_index], w_out[layer_index])
            return ((jnp.maximum(act_peak, normed_peak), jnp.maximum(head_peak, attended_peak)), output)
        start_peaks = (jnp.zeros((D,), jnp.float32), jnp.zeros((HEADS * HEAD_DIM,), jnp.float32))
        (act_peak, head_peak), stream = lax.scan(advance, start_peaks, stream)
        outputs.append(stream)
        weight_peak = jnp.maximum(jnp.maximum(lax.optimization_barrier(jnp.max(jnp.abs(w_query[layer_index]), axis=1)), lax.optimization_barrier(jnp.max(jnp.abs(w_key[layer_index]), axis=1))), lax.optimization_barrier(jnp.max(jnp.abs(w_value[layer_index]), axis=1))).astype(jnp.float32)
        out_peak = lax.optimization_barrier(jnp.max(jnp.abs(w_out[layer_index]), axis=1)).astype(jnp.float32)
        scale_in = smoothing(act_peak, weight_peak, alpha_exp)
        scale_out = smoothing(head_peak, out_peak, alpha_exp)
        inputs_scales.append(scale_in)
        output_scales.append(scale_out)
        smooth_query.append((w_query[layer_index].astype(jnp.float32) * scale_in[:, None]).astype(jnp.bfloat16))
        smooth_key.append((w_key[layer_index].astype(jnp.float32) * scale_in[:, None]).astype(jnp.bfloat16))
        smooth_value.append((w_value[layer_index].astype(jnp.float32) * scale_in[:, None]).astype(jnp.bfloat16))
    return (jnp.stack(outputs), jnp.stack(inputs_scales), jnp.stack(output_scales), jnp.stack(smooth_query), jnp.stack(smooth_key), jnp.stack(smooth_value))
```

```python
import math

import jax
import jax.numpy as jnp
from jax import lax
from jax.sharding import Mesh
from jax.sharding import PartitionSpec as P

KV_HEADS = 4
HEAD_DIM = 128
TP = ("x", "z")
SECTION = ("y", "core")
N_Y = 4
N_CORE = 2
N_TP = 16

norm_eps = 1e-05
stat_eps = 1e-05
rope_base = 500000.0


def copy_for_each(value, axis):
    count = lax.axis_size(axis)
    return lax.all_to_all(
        jnp.broadcast_to(value[None], (count, *value.shape)), axis, 0, 0, tiled=True
    )


def rope_tables(length, head_size):
    halves = head_size // 2
    freqs = jnp.exp(-math.log(rope_base) * 2.0 * jnp.arange(halves, dtype=jnp.float32) / head_size)
    angles = jnp.arange(length, dtype=jnp.float32)[:, None] * freqs[None, :]
    return (jnp.cos(angles), jnp.sin(angles))


def smoothing(act_peak, weight_peak, alpha_exp):
    return jnp.exp(
        alpha_exp * jnp.log(act_peak + stat_eps)
        - (1.0 - alpha_exp) * jnp.log(weight_peak + stat_eps)
    )


def shards(token_ids, alpha_num, embed_table, norm_gain, w_query, w_key, w_value, w_out):
    bf16, f32 = jnp.bfloat16, jnp.float32
    y_index = lax.axis_index("y")
    core_index = lax.axis_index("core")
    section_index = lax.axis_index(SECTION)
    tp_index = lax.axis_index(TP)
    micros, length = token_ids.shape
    vocab_rows = embed_table.shape[0]
    layers = N_Y * N_CORE
    own_rows = length // N_TP
    width = w_query.shape[1]
    part = width // N_Y
    query_cols = w_query.shape[2]
    kv_cols = w_key.shape[2]
    heads_here = query_cols // HEAD_DIM

    kv_turned = jnp.concatenate([w_key[0].T, w_value[0].T], axis=0)
    kv_blocks = kv_turned.reshape(2 * kv_cols, N_Y, part).transpose(1, 0, 2)
    out_blocks = w_out[0].reshape(query_cols, N_Y, part).transpose(1, 0, 2)
    swap = [(0, 1), (1, 0)]
    own_q = lax.all_to_all(w_query[0].reshape(N_Y, part, query_cols), "y", 0, 0, tiled=True)
    own_kv = lax.all_to_all(kv_blocks, "y", 0, 0, tiled=True)
    own_out = lax.all_to_all(out_blocks, "y", 0, 0, tiled=True)
    twin_q = lax.ppermute(own_q, "core", swap)
    twin_kv = lax.ppermute(own_kv, "core", swap)
    twin_out = lax.ppermute(own_out, "core", swap)
    gains = copy_for_each(norm_gain[0], SECTION)
    gains = lax.dynamic_slice_in_dim(gains, y_index * part, part, axis=1)

    local_ids = token_ids - section_index * vocab_rows
    inside = (local_ids >= 0) & (local_ids < vocab_rows)
    picked = jnp.take(embed_table, jnp.clip(local_ids, 0, vocab_rows - 1), axis=0)
    picked = jnp.where(inside[:, :, None], picked, jnp.zeros((), bf16))
    feats = embed_table.shape[1]
    sent = picked.reshape(micros, N_TP, own_rows, feats).transpose(1, 0, 2, 3)
    came = lax.all_to_all(sent, TP, 0, 0, tiled=True)
    came = came.reshape(N_Y, N_TP // N_Y, micros, own_rows, feats).transpose(0, 2, 3, 1, 4)
    found = lax.all_to_all(came.reshape(layers, own_rows, part), SECTION, 0, 0, tiled=True)
    resid = jnp.sum(found.astype(f32), axis=0).astype(bf16)

    weight_local = jnp.maximum(
        jnp.max(jnp.abs(w_query[0]), axis=1),
        jnp.maximum(jnp.max(jnp.abs(w_key[0]), axis=1), jnp.max(jnp.abs(w_value[0]), axis=1)),
    )
    out_peak = jnp.max(jnp.abs(w_out[0]), axis=1).astype(f32)

    cosine, sine = rope_tables(length, HEAD_DIM)
    cosine_t, sine_t = cosine.T, sine.T
    positions = jnp.arange(length, dtype=jnp.int32)
    causal = positions[:, None] >= positions[None, :]
    kv_half = tp_index % 2
    per_half = N_TP // 2

    weight_peak = None
    stored, act_peaks, head_peaks = [], [], []
    for layer in range(layers):
        plane, side = divmod(layer, N_CORE)
        mine = core_index == side
        weight_q = jnp.where(mine, own_q[plane], twin_q[plane])
        weight_kv = jnp.where(mine, own_kv[plane], twin_kv[plane])
        weight_out = jnp.where(mine, own_out[plane], twin_out[plane])
        if layer == 0:
            rows = weight_local.reshape(-1, part)
            both = copy_for_each(jnp.concatenate([resid, rows], axis=0), TP)
            gathered = both[:, :own_rows].reshape(length, part)
            weight_peak = jnp.max(both[:, own_rows:], axis=0).reshape(width).astype(f32)
        else:
            gathered = copy_for_each(resid, TP).reshape(length, part)
        values = gathered.astype(f32)
        scaled = values * gains[layer][None, :]
        square = jnp.sum(values * values, axis=1)
        high = lax.reduce_precision(square, 8, 7)
        low = square - high
        lhs = scaled.astype(bf16)
        query_part = jnp.dot(lhs, weight_q, preferred_element_type=f32).astype(bf16)
        kv_part = lax.dot_general(
            weight_kv, lhs, (((1,), (1,)), ((), ())), preferred_element_type=f32
        ).astype(bf16)
        pieces = [query_part[:, h * HEAD_DIM : (h + 1) * HEAD_DIM] for h in range(heads_here)]
        stats = jnp.concatenate(
            [high[None, :], low[None, :], jnp.zeros((6, length), f32)], axis=0
        ).astype(bf16)
        packed = jnp.concatenate([*pieces, kv_part, stats], axis=0)
        summed = jnp.sum(copy_for_each(packed, "y").astype(f32), axis=0)
        kv_at = heads_here * length
        stat_at = kv_at + 2 * kv_cols
        mean = (summed[stat_at] + summed[stat_at + 1]) / width
        inverse = lax.rsqrt(mean + norm_eps)
        kv_rows = (summed[kv_at:stat_at] * inverse[None, :]).astype(bf16)
        normed = (scaled * inverse[:, None]).astype(bf16)
        act_peaks.append(jnp.max(jnp.abs(normed), axis=0))

        kv_all = copy_for_each(kv_rows, TP)
        kv_all = lax.dynamic_slice_in_dim(kv_all, kv_half * per_half, per_half, axis=0)
        kv_all = kv_all.reshape(heads_here, KV_HEADS, 2, kv_cols, length)
        parts = []
        for h in range(heads_here):
            key_t = kv_all[h, :, 0].reshape(HEAD_DIM, length).astype(f32)
            value_t = kv_all[h, :, 1].reshape(HEAD_DIM, length)
            halves = HEAD_DIM // 2
            low_k, high_k = key_t[:halves], key_t[halves:]
            key_rot = jnp.concatenate(
                [low_k * cosine_t - high_k * sine_t, high_k * cosine_t + low_k * sine_t], axis=0
            ).astype(bf16)
            query = summed[h * length : (h + 1) * length] * inverse[:, None]
            low_q, high_q = query[:, :halves], query[:, halves:]
            query_rot = jnp.concatenate(
                [low_q * cosine - high_q * sine, high_q * cosine + low_q * sine], axis=1
            ).astype(bf16)
            scores = jnp.dot(query_rot, key_rot, preferred_element_type=f32) / math.sqrt(HEAD_DIM)
            scores = jnp.where(causal, scores, -1e30)
            probs = jax.nn.softmax(scores, axis=-1).astype(bf16)
            parts.append(
                lax.dot_general(
                    probs, value_t, (((1,), (1,)), ((), ())), preferred_element_type=f32
                ).astype(bf16)
            )
        attended = jnp.concatenate(parts, axis=1)
        head_peaks.append(jnp.max(jnp.abs(attended), axis=0))
        head_part = jnp.dot(attended, weight_out, preferred_element_type=f32).astype(bf16)
        shares = lax.all_to_all(
            head_part.reshape(N_TP, own_rows, part), TP, 0, 0, tiled=True
        )
        mixed = jnp.sum(shares.astype(f32), axis=0)
        resid = (resid.astype(f32) + mixed).astype(bf16)
        stored.append(resid)

    peaks = jnp.concatenate([jnp.stack(act_peaks), jnp.stack(head_peaks)], axis=1)
    peaks = lax.all_to_all(peaks, SECTION, 0, 0, tiled=True).astype(f32)
    peaks = peaks.reshape(N_Y, N_CORE, part + query_cols).max(axis=1)
    act_peak = peaks[:, :part].reshape(width)
    head_peak = peaks[0, part:]
    kept = lax.all_to_all(jnp.stack(stored), SECTION, 0, 0, tiled=True)
    kept = kept.reshape(N_Y, N_CORE, own_rows, part).transpose(1, 2, 0, 3)
    kept = kept.reshape(micros, own_rows, width)

    alpha_exp = alpha_num[0].astype(f32) / 10.0
    scale_in = smoothing(act_peak, weight_peak, alpha_exp)
    scale_out = smoothing(head_peak, out_peak, alpha_exp)
    smooth_query, smooth_key, smooth_value = (
        (w.astype(f32) * scale_in[None, :, None]).astype(bf16) for w in (w_query, w_key, w_value)
    )
    return (kept[None], scale_in[None], scale_out[None], smooth_query, smooth_key, smooth_value)


def solution(mesh):
    split = Mesh(mesh.devices.reshape(N_Y, N_CORE, 4, 4), ("y", "core", "x", "z"))
    return jax.shard_map(
        shards,
        mesh=split,
        in_specs=(
            P(),
            P(),
            P(SECTION, TP),
            P(SECTION, None),
            P(SECTION, None, TP),
            P(SECTION, None, TP),
            P(SECTION, None, TP),
            P(SECTION, TP, None),
        ),
        out_specs=(
            P(SECTION, None, TP, None),
            P(SECTION, None),
            P(SECTION, TP),
            P(SECTION, None, TP),
            P(SECTION, None, TP),
            P(SECTION, None, TP),
        ),
        check_vma=False,
    )
```

```python
import math

import jax
import jax.numpy as jnp
from jax import lax
from jax.experimental import pallas as pl
from jax.experimental.pallas import tpu as pltpu
from jax.sharding import Mesh
from jax.sharding import PartitionSpec as P

KV_HEADS = 4
HEAD_DIM = 128
TP = ("x", "zh", "zl")
HALF = ("x", "zh")
SECTION = ("y", "core")
N_Y = 4
N_CORE = 2
N_TP = 16
GAIN_ROWS = 16

norm_eps = 1e-05
stat_eps = 1e-05
rope_base = 500000.0


def copy_for_each(value, axis):
    count = lax.axis_size(axis)
    return lax.all_to_all(
        jnp.broadcast_to(value[None], (count, *value.shape)), axis, 0, 0, tiled=True
    )


def rope_tables(length, head_size):
    halves = head_size // 2
    freqs = jnp.exp(-math.log(rope_base) * 2.0 * jnp.arange(halves, dtype=jnp.float32) / head_size)
    angles = jnp.arange(length, dtype=jnp.float32)[:, None] * freqs[None, :]
    return (jnp.cos(angles), jnp.sin(angles))


def smoothing(act_peak, weight_peak, alpha_exp):
    return jnp.exp(
        alpha_exp * jnp.log(act_peak + stat_eps)
        - (1.0 - alpha_exp) * jnp.log(weight_peak + stat_eps)
    )


def fetch(choice, sources, target, sem):
    for number, source in enumerate(sources):

        @pl.when(choice == number)
        def _():
            pltpu.make_async_copy(source, target, sem).start()


def front_body(choice_ref, x_ref, *refs):
    count = 2 * N_Y
    q_refs, kv_refs = refs[:count], refs[count : 2 * count]
    out_ref, q_buf, kv_buf, sems = refs[2 * count :]
    choice = choice_ref[0]
    fetch(choice, kv_refs, kv_buf, sems.at[0])
    fetch(choice, q_refs, q_buf, sems.at[1])
    values = x_ref[...].astype(jnp.float32)
    length, part = values.shape
    square = jnp.sum(values * values, axis=1, keepdims=True)
    square = jnp.broadcast_to(square, (length, HEAD_DIM)).T[:8]
    high = square.astype(jnp.bfloat16)
    low = (square - high.astype(jnp.float32)).astype(jnp.bfloat16)
    pltpu.make_async_copy(kv_refs[0], kv_buf, sems.at[0]).wait()
    rows = kv_buf.shape[0] - GAIN_ROWS
    gain = kv_buf[rows:, :].astype(jnp.float32)
    gain = jnp.sum(gain, axis=0, keepdims=True)
    lhs = (values * gain).astype(jnp.bfloat16)
    kv_part = lax.dot_general(
        kv_buf[:rows, :], lhs, (((1,), (1,)), ((), ())), preferred_element_type=jnp.float32
    ).astype(jnp.bfloat16)
    pltpu.make_async_copy(q_refs[0], q_buf, sems.at[1]).wait()
    query = jnp.dot(lhs, q_buf[...], preferred_element_type=jnp.float32).astype(jnp.bfloat16)
    heads = query.shape[1] // HEAD_DIM
    for copy in range(N_Y):
        for h in range(heads):
            out_ref[copy, h * length : (h + 1) * length, :] = query[
                :, h * HEAD_DIM : (h + 1) * HEAD_DIM
            ]
        at = heads * length
        out_ref[copy, at : at + rows, :] = kv_part
        out_ref[copy, at + rows : at + rows + 8, :] = high
        out_ref[copy, at + rows + 8 :, :] = low


def back_body(
    choice_ref, x_ref, sums_ref, kv_ref, gains_ref, cos_ref, sin_ref, cos_t_ref, sin_t_ref, *refs
):
    f32, bf16 = jnp.float32, jnp.bfloat16
    count = 2 * N_Y
    w_refs = refs[:count]
    out_ref, peaks_ref, w_buf, sem = refs[count:]
    choice = choice_ref[0]
    fetch(choice, w_refs, w_buf, sem)
    length, part = x_ref.shape
    query_cols = w_buf.shape[0]
    heads = query_cols // HEAD_DIM
    pieces = kv_ref.shape[0] // heads
    kv_cols = kv_ref.shape[1] // 2
    stat_at = heads * length + 2 * kv_cols
    square = sums_ref[stat_at : stat_at + 1, :] + sums_ref[stat_at + 8 : stat_at + 9, :]
    inverse = lax.rsqrt(square / (part * N_Y) + norm_eps)
    inverse = jnp.broadcast_to(inverse, (HEAD_DIM, length)).T
    rows = lax.broadcasted_iota(jnp.int32, (length, length), 0)
    cols = lax.broadcasted_iota(jnp.int32, (length, length), 1)
    halves = HEAD_DIM // 2
    outs = []
    for h in range(heads):
        of_head = [kv_ref[h * pieces + piece] for piece in range(pieces)]
        key_t = jnp.concatenate([piece[:kv_cols] for piece in of_head], axis=0).astype(f32)
        value_t = jnp.concatenate([piece[kv_cols:] for piece in of_head], axis=0)
        turned = jnp.concatenate([key_t[halves:], key_t[:halves]], axis=0)
        key_rot = (key_t * cos_t_ref[...] + turned * sin_t_ref[...]).astype(bf16)
        query = sums_ref[h * length : (h + 1) * length, :] * inverse
        query_rot = query * cos_ref[...] + pltpu.roll(query, halves, 1) * sin_ref[...]
        scores = jnp.dot(query_rot.astype(bf16), key_rot, preferred_element_type=f32)
        scores = jnp.where(rows >= cols, scores / math.sqrt(HEAD_DIM), -1e30)
        scores = jnp.exp(scores - jnp.max(scores, axis=1, keepdims=True))
        probs = (scores / jnp.sum(scores, axis=1, keepdims=True)).astype(bf16)
        outs.append(
            lax.dot_general(
                probs, value_t, (((1,), (1,)), ((), ())), preferred_element_type=f32
            ).astype(bf16)
        )
    attended = jnp.concatenate(outs, axis=1)
    peaks_ref[:, part:] = jnp.max(jnp.abs(attended.astype(f32)), axis=0, keepdims=True)
    for at in range(0, part, HEAD_DIM):
        block = x_ref[:, at : at + HEAD_DIM].astype(f32)
        gain = gains_ref[choice, :, at : at + HEAD_DIM]
        normed = (block * inverse * gain).astype(bf16).astype(f32)
        peaks_ref[:, at : at + HEAD_DIM] = jnp.max(jnp.abs(normed), axis=0, keepdims=True)
    pltpu.make_async_copy(w_refs[0], w_buf, sem).wait()
    out_ref[...] = jnp.dot(attended, w_buf[...], preferred_element_type=f32).astype(bf16)


def front(choice, gathered, blocks_q, blocks_kv):
    length = gathered.shape[0]
    rows = blocks_q[0].shape[1] + blocks_kv[0].shape[0]
    hbm = pl.BlockSpec(memory_space=pl.ANY)
    vmem = pl.BlockSpec(memory_space=pltpu.VMEM)
    return pl.pallas_call(
        front_body,
        out_shape=jax.ShapeDtypeStruct((N_Y, rows, length), jnp.bfloat16),
        in_specs=[pl.BlockSpec(memory_space=pltpu.SMEM), vmem, *[hbm] * (4 * N_Y)],
        out_specs=vmem,
        scratch_shapes=[
            pltpu.VMEM(blocks_q[0].shape, jnp.bfloat16),
            pltpu.VMEM(blocks_kv[0].shape, jnp.bfloat16),
            pltpu.SemaphoreType.DMA((2,)),
        ],
        compiler_params=pltpu.CompilerParams(vmem_limit_bytes=16 << 20),
        name="front",
    )(choice, gathered, *blocks_q, *blocks_kv)


def back(choice, gathered, sums, kv_all, gains, tables, blocks):
    length, part = gathered.shape
    hbm = pl.BlockSpec(memory_space=pl.ANY)
    vmem = pl.BlockSpec(memory_space=pltpu.VMEM)
    return pl.pallas_call(
        back_body,
        out_shape=(
            jax.ShapeDtypeStruct((length, part), jnp.bfloat16),
            jax.ShapeDtypeStruct((1, part + blocks[0].shape[0]), jnp.float32),
        ),
        in_specs=[
            pl.BlockSpec(memory_space=pltpu.SMEM),
            *[vmem] * 8,
            *[hbm] * (2 * N_Y),
        ],
        out_specs=(vmem, vmem),
        scratch_shapes=[
            pltpu.VMEM(blocks[0].shape, jnp.bfloat16),
            pltpu.SemaphoreType.DMA(()),
        ],
        compiler_params=pltpu.CompilerParams(vmem_limit_bytes=16 << 20),
        name="back",
    )(choice, gathered, sums, kv_all, gains, *tables, *blocks)


def shards(token_ids, alpha_num, embed_table, norm_gain, w_query, w_key, w_value, w_out):
    bf16, f32 = jnp.bfloat16, jnp.float32
    y_index = lax.axis_index("y")
    core_index = lax.axis_index("core")
    section_index = lax.axis_index(SECTION)
    micros, length = token_ids.shape
    vocab_rows = embed_table.shape[0]
    layers = N_Y * N_CORE
    own_rows = length // N_TP
    width = w_query.shape[1]
    part = width // N_Y
    query_cols = w_query.shape[2]
    kv_cols = w_key.shape[2]
    heads_here = query_cols // HEAD_DIM

    swap = [(0, 1), (1, 0)]

    def spread(block_for):
        own = {}
        for step in (0, 1, 3, 2):
            block = block_for((y_index + step) % N_Y)
            if step:
                block = lax.ppermute(block, "y", [(i, (i + step) % N_Y) for i in range(N_Y)])
            own[step] = block
        twins = [lax.ppermute(own[step], "core", swap) for step in range(N_Y)]
        return [*[own[step] for step in range(N_Y)], *twins]

    kv_turned = jnp.concatenate([w_key[0].T, w_value[0].T], axis=0)
    routes = []
    for source in range(N_TP):
        half, place = divmod(source, N_TP // 2)
        routes.append((source, place * 2 + half))
    kv_turned = lax.ppermute(kv_turned, TP, routes)
    gain = norm_gain[0]
    gain_high = lax.reduce_precision(gain, 8, 7)
    gain_mid = lax.reduce_precision(gain - gain_high, 8, 7)
    gain_low = gain - gain_high - gain_mid
    gain_rows = jnp.stack([gain_high, gain_mid, gain_low]).astype(bf16)
    kv_turned = jnp.concatenate([kv_turned, jnp.pad(gain_rows, ((0, GAIN_ROWS - 3), (0, 0)))], axis=0)

    blocks_q = spread(
        lambda block: lax.dynamic_slice_in_dim(w_query[0], block * part, part, axis=0)
    )
    blocks_kv = spread(
        lambda block: lax.dynamic_slice_in_dim(kv_turned, block * part, part, axis=1)
    )
    local_ids = token_ids - section_index * vocab_rows
    inside = (local_ids >= 0) & (local_ids < vocab_rows)
    picked = jnp.take(embed_table, jnp.clip(local_ids, 0, vocab_rows - 1), axis=0)
    picked = jnp.where(inside[:, :, None], picked, jnp.zeros((), bf16))
    feats = embed_table.shape[1]
    sent = picked.reshape(micros, N_TP, own_rows, feats).transpose(1, 0, 2, 3)
    came = lax.all_to_all(sent, TP, 0, 0, tiled=True)
    came = came.reshape(N_Y, N_TP // N_Y, micros, own_rows, feats).transpose(0, 2, 3, 1, 4)
    found = lax.all_to_all(came.reshape(layers, own_rows, part), SECTION, 0, 0, tiled=True)
    resid = jnp.sum(found.astype(f32), axis=0).astype(bf16)

    late_out, resid = lax.optimization_barrier((w_out[0], resid))
    blocks_out = spread(
        lambda block: lax.dynamic_slice_in_dim(late_out, block * part, part, axis=1)
    )

    seen_q, seen_k, seen_v, seen_out, _ = lax.optimization_barrier(
        (w_query[0], w_key[0], w_value[0], w_out[0], came)
    )
    weight_local = jnp.maximum(
        jnp.max(jnp.abs(seen_q), axis=1),
        jnp.maximum(jnp.max(jnp.abs(seen_k), axis=1), jnp.max(jnp.abs(seen_v), axis=1)),
    )
    out_peak = jnp.max(jnp.abs(seen_out), axis=1).astype(f32)

    cosine, sine = rope_tables(length, HEAD_DIM)
    cosine = jnp.concatenate([cosine, cosine], axis=1)
    sine = jnp.concatenate([-sine, sine], axis=1)
    tables = (cosine, sine, cosine.T, sine.T)
    numbers = jnp.arange(layers, dtype=jnp.int32)
    steps = (y_index - numbers // N_CORE) % N_Y
    choices = jnp.where(numbers % N_CORE == core_index, steps, steps + N_Y).astype(jnp.int32)

    gains = [jnp.sum(block[2 * kv_cols :].astype(f32), axis=0) for block in blocks_kv]
    gains = jnp.stack(gains)[:, None, :]
    kv_at = heads_here * length
    stat_at = kv_at + 2 * kv_cols

    def one_layer(layer, gathered, resid):
        choice = lax.dynamic_slice_in_dim(choices, layer, 1)
        choice, gathered = lax.optimization_barrier((choice, gathered))
        packed = front(choice, gathered, blocks_q, blocks_kv)
        summed = jnp.sum(lax.all_to_all(packed, "y", 0, 0, tiled=True).astype(f32), axis=0)
        mean = (summed[stat_at] + summed[stat_at + 8]) / width
        inverse = lax.rsqrt(mean + norm_eps)
        kv_rows = (summed[kv_at:stat_at] * inverse[None, :]).astype(bf16)
        kv_all = copy_for_each(kv_rows, HALF)
        head_part, peaks = back(choice, gathered, summed, kv_all, gains, tables, blocks_out)
        shares = lax.all_to_all(head_part.reshape(N_TP, own_rows, part), TP, 0, 0, tiled=True)
        shares, peaks = lax.optimization_barrier((shares, peaks))
        mixed = jnp.sum(shares.astype(f32), axis=0)
        return (resid.astype(f32) + mixed).astype(bf16), peaks

    rows = weight_local.reshape(-1, part)
    both = copy_for_each(jnp.concatenate([resid, rows], axis=0), TP)
    weight_peak = jnp.max(both[:, own_rows:], axis=0).reshape(width).astype(f32)
    resid, first_peaks = one_layer(jnp.int32(0), both[:, :own_rows].reshape(length, part), resid)

    def advance(layer, carry):
        resid, stored, peaks = carry
        gathered = copy_for_each(resid, TP).reshape(length, part)
        resid, fresh = one_layer(layer, gathered, resid)
        stored = lax.dynamic_update_index_in_dim(stored, resid, layer, 0)
        peaks = lax.dynamic_update_slice_in_dim(peaks, fresh, layer, 0)
        return resid, stored, peaks

    stored = jnp.zeros((layers, own_rows, part), bf16).at[0].set(resid)
    peaks = jnp.zeros((layers, part + query_cols), f32).at[0].set(first_peaks[0])
    resid, stored, peaks = lax.fori_loop(1, layers, advance, (resid, stored, peaks))

    peaks = lax.all_to_all(peaks.astype(bf16), SECTION, 0, 0, tiled=True).astype(f32)
    peaks = peaks.reshape(N_Y, N_CORE, part + query_cols).max(axis=1)
    act_peak = peaks[:, :part].reshape(width)
    head_peak = peaks[0, part:]
    kept = lax.all_to_all(stored, SECTION, 0, 0, tiled=True)
    kept = kept.reshape(N_Y, N_CORE, own_rows, part).transpose(1, 2, 0, 3)
    kept = kept.reshape(micros, own_rows, width)

    alpha_exp = alpha_num[0].astype(f32) / 10.0
    scale_in = smoothing(act_peak, weight_peak, alpha_exp)
    scale_out = smoothing(head_peak, out_peak, alpha_exp)
    smooth_query, smooth_key, smooth_value = (
        (w.astype(f32) * scale_in[None, :, None]).astype(bf16) for w in (w_query, w_key, w_value)
    )
    return (kept[None], scale_in[None], scale_out[None], smooth_query, smooth_key, smooth_value)


def solution(mesh):
    split = Mesh(mesh.devices.reshape(N_Y, N_CORE, 4, 2, 2), ("y", "core", "x", "zh", "zl"))
    return jax.shard_map(
        shards,
        mesh=split,
        in_specs=(
            P(),
            P(),
            P(SECTION, TP),
            P(SECTION, None),
            P(SECTION, None, TP),
            P(SECTION, None, TP),
            P(SECTION, None, TP),
            P(SECTION, TP, None),
        ),
        out_specs=(
            P(SECTION, None, TP, None),
            P(SECTION, None),
            P(SECTION, TP),
            P(SECTION, None, TP),
            P(SECTION, None, TP),
            P(SECTION, None, TP),
        ),
        check_vma=False,
    )
```

```python
import math

import jax
import jax.numpy as jnp
from jax import lax
from jax.experimental import pallas as pl
from jax.experimental.pallas import tpu as pltpu
from jax.sharding import Mesh
from jax.sharding import PartitionSpec as P


HEAD_DIM = 128
TP = ("x", "zh", "zl")
HALF = ("x", "zh")
SECTION = ("y", "core")
N_Y = 4
N_CORE = 2
N_TP = 16
GAIN_ROWS = 16

norm_eps = 1e-05
stat_eps = 1e-05
rope_base = 500000.0


def copy_for_each(value, axis):
    count = lax.axis_size(axis)
    return lax.all_to_all(
        jnp.broadcast_to(value[None], (count, *value.shape)), axis, 0, 0, tiled=True
    )


def rope_tables(length, head_size):
    halves = head_size // 2
    freqs = jnp.exp(-math.log(rope_base) * 2.0 * jnp.arange(halves, dtype=jnp.float32) / head_size)
    angles = jnp.arange(length, dtype=jnp.float32)[:, None] * freqs[None, :]
    return (jnp.cos(angles), jnp.sin(angles))


def smoothing(act_peak, weight_peak, alpha_exp):
    return jnp.exp(
        alpha_exp * jnp.log(act_peak + stat_eps)
        - (1.0 - alpha_exp) * jnp.log(weight_peak + stat_eps)
    )


def fetch(choice, sources, target, sem):
    for number, source in enumerate(sources):

        @pl.when(choice == number)
        def _():
            pltpu.make_async_copy(source, target, sem).start()


def choice_of(state_ref):
    layer = state_ref[0]
    step = (state_ref[1] - layer // N_CORE + N_Y) % N_Y
    return jnp.where(layer % N_CORE == state_ref[2], step, step + N_Y)


def front_body(state_ref, x_ref, *refs):
    count = 2 * N_Y
    q_refs, kv_refs = refs[:count], refs[count : 2 * count]
    out_ref, q_buf, kv_buf, sems = refs[2 * count :]
    choice = choice_of(state_ref)
    fetch(choice, kv_refs, kv_buf, sems.at[0])
    fetch(choice, q_refs, q_buf, sems.at[1])
    values = x_ref[...].astype(jnp.float32)
    length, _ = values.shape
    square = jnp.sum(values * values, axis=1, keepdims=True)
    square = jnp.broadcast_to(square, (length, HEAD_DIM)).T[:8]
    high = square.astype(jnp.bfloat16)
    low = (square - high.astype(jnp.float32)).astype(jnp.bfloat16)
    pltpu.make_async_copy(kv_refs[0], kv_buf, sems.at[0]).wait()
    rows = kv_buf.shape[0] - GAIN_ROWS
    gain = kv_buf[rows:, :].astype(jnp.float32)
    gain = jnp.sum(gain, axis=0, keepdims=True)
    lhs = (values * gain).astype(jnp.bfloat16)
    kv_part = lax.dot_general(
        kv_buf[:rows, :], lhs, (((1,), (1,)), ((), ())), preferred_element_type=jnp.float32
    ).astype(jnp.bfloat16)
    pltpu.make_async_copy(q_refs[0], q_buf, sems.at[1]).wait()
    query = jnp.dot(lhs, q_buf[...], preferred_element_type=jnp.float32).astype(jnp.bfloat16)
    heads = query.shape[1] // HEAD_DIM
    for copy in range(N_Y):
        for h in range(heads):
            out_ref[copy, h * length : (h + 1) * length, :] = query[
                :, h * HEAD_DIM : (h + 1) * HEAD_DIM
            ]
        at = heads * length
        out_ref[copy, at : at + rows, :] = kv_part
        out_ref[copy, at + rows : at + rows + 8, :] = high
        out_ref[copy, at + rows + 8 :, :] = low


def back_body(
    state_ref, x_ref, sums_ref, kv_ref, cos_ref, sin_ref, cos_t_ref, sin_t_ref, *refs
):
    f32, bf16 = jnp.float32, jnp.bfloat16
    count = 2 * N_Y
    w_refs, g_refs = refs[:count], refs[count : 2 * count]
    out_ref, peaks_ref, w_buf, g_buf, sems = refs[2 * count :]
    choice = choice_of(state_ref)
    first_gain = g_refs[0].shape[0] - GAIN_ROWS
    g_refs = [ref.at[pl.ds(first_gain, GAIN_ROWS), :] for ref in g_refs]
    fetch(choice, g_refs, g_buf, sems.at[0])
    fetch(choice, w_refs, w_buf, sems.at[1])
    length, part = x_ref.shape
    query_cols = w_buf.shape[0]
    heads = query_cols // HEAD_DIM
    pieces = kv_ref.shape[0] // heads
    kv_cols = kv_ref.shape[1] // 2
    stat_at = heads * length + 2 * kv_cols
    square = sums_ref[stat_at : stat_at + 1, :] + sums_ref[stat_at + 8 : stat_at + 9, :]
    inverse = lax.rsqrt(square / (part * N_Y) + norm_eps)
    inverse = jnp.broadcast_to(inverse, (HEAD_DIM, length)).T
    rows = lax.broadcasted_iota(jnp.int32, (length, length), 0)
    cols = lax.broadcasted_iota(jnp.int32, (length, length), 1)
    halves = HEAD_DIM // 2
    outs = []
    for h in range(heads):
        of_head = [kv_ref[h * pieces + (piece ^ 1)] for piece in range(pieces)]
        key_t = jnp.concatenate([piece[:kv_cols] for piece in of_head], axis=0).astype(f32)
        value_t = jnp.concatenate([piece[kv_cols:] for piece in of_head], axis=0)
        turned = jnp.concatenate([key_t[halves:], key_t[:halves]], axis=0)
        key_rot = (key_t * cos_t_ref[...] + turned * sin_t_ref[...]).astype(bf16)
        query = sums_ref[h * length : (h + 1) * length, :] * inverse
        query_rot = query * cos_ref[...] + pltpu.roll(query, halves, 1) * sin_ref[...]
        scores = jnp.dot(query_rot.astype(bf16), key_rot, preferred_element_type=f32)
        scores = jnp.where(rows >= cols, scores / math.sqrt(HEAD_DIM), -1e30)
        scores = jnp.exp(scores - jnp.max(scores, axis=1, keepdims=True))
        probs = (scores / jnp.sum(scores, axis=1, keepdims=True)).astype(bf16)
        outs.append(
            lax.dot_general(
                probs, value_t, (((1,), (1,)), ((), ())), preferred_element_type=f32
            ).astype(bf16)
        )
    attended = jnp.concatenate(outs, axis=1)
    peaks_ref[:, part:] = jnp.max(jnp.abs(attended.astype(f32)), axis=0, keepdims=True)
    pltpu.make_async_copy(g_refs[0], g_buf, sems.at[0]).wait()
    for at in range(0, part, HEAD_DIM):
        block = x_ref[:, at : at + HEAD_DIM].astype(f32)
        gain = g_buf[:, at : at + HEAD_DIM].astype(f32)
        gain = jnp.sum(gain, axis=0, keepdims=True)
        normed = (block * inverse * gain).astype(bf16).astype(f32)
        peaks_ref[:, at : at + HEAD_DIM] = jnp.max(jnp.abs(normed), axis=0, keepdims=True)
    pltpu.make_async_copy(w_refs[0], w_buf, sems.at[1]).wait()
    out_ref[...] = jnp.dot(attended, w_buf[...], preferred_element_type=f32).astype(bf16)


def front(state, gathered, blocks_q, blocks_kv):
    length = gathered.shape[0]
    rows = blocks_q[0].shape[1] + blocks_kv[0].shape[0]
    hbm = pl.BlockSpec(memory_space=pl.ANY)
    vmem = pl.BlockSpec(memory_space=pltpu.VMEM)
    return pl.pallas_call(
        front_body,
        out_shape=jax.ShapeDtypeStruct((N_Y, rows, length), jnp.bfloat16),
        in_specs=[pl.BlockSpec(memory_space=pltpu.SMEM), vmem, *[hbm] * (4 * N_Y)],
        out_specs=vmem,
        scratch_shapes=[
            pltpu.VMEM(blocks_q[0].shape, jnp.bfloat16),
            pltpu.VMEM(blocks_kv[0].shape, jnp.bfloat16),
            pltpu.SemaphoreType.DMA((2,)),
        ],
        compiler_params=pltpu.CompilerParams(vmem_limit_bytes=16 << 20),
        name="front",
    )(state, gathered, *blocks_q, *blocks_kv)


def back(state, gathered, sums, kv_all, tables, blocks, blocks_kv):
    length, part = gathered.shape
    hbm = pl.BlockSpec(memory_space=pl.ANY)
    vmem = pl.BlockSpec(memory_space=pltpu.VMEM)
    return pl.pallas_call(
        back_body,
        out_shape=(
            jax.ShapeDtypeStruct((length, part), jnp.bfloat16),
            jax.ShapeDtypeStruct((1, part + blocks[0].shape[0]), jnp.float32),
        ),
        in_specs=[
            pl.BlockSpec(memory_space=pltpu.SMEM),
            *[vmem] * 7,
            *[hbm] * (4 * N_Y),
        ],
        out_specs=(vmem, vmem),
        scratch_shapes=[
            pltpu.VMEM(blocks[0].shape, jnp.bfloat16),
            pltpu.VMEM((GAIN_ROWS, part), jnp.bfloat16),
            pltpu.SemaphoreType.DMA((2,)),
        ],
        compiler_params=pltpu.CompilerParams(vmem_limit_bytes=16 << 20),
        name="back",
    )(state, gathered, sums, kv_all, *tables, *blocks, *blocks_kv)


def program(token_ids, alpha_num, embed_table, norm_gain, w_query, w_key, w_value, w_out):
    bf16, f32 = jnp.bfloat16, jnp.float32
    y_index = lax.axis_index("y")
    core_index = lax.axis_index("core")
    section_index = lax.axis_index(SECTION)
    micros, length = token_ids.shape
    vocab_rows = embed_table.shape[0]
    layers = N_Y * N_CORE
    own_rows = length // N_TP
    width = w_query.shape[1]
    part = width // N_Y
    query_cols = w_query.shape[2]
    kv_cols = w_key.shape[2]
    heads_here = query_cols // HEAD_DIM

    swap = [(0, 1), (1, 0)]

    def spread(block_for, after=None):
        own = {step: block_for((y_index + step) % N_Y) for step in (0, 1, 3, 2)}
        if after is not None:
            own, _ = lax.optimization_barrier((own, after))
        for step in (1, 3, 2):
            turn = [(i, (i + step) % N_Y) for i in range(N_Y)]
            own[step] = lax.ppermute(own[step], "y", turn)
        twins = []
        for step in range(N_Y):
            twins.append(lax.ppermute(own[step], "core", swap))
        return [*[own[step] for step in range(N_Y)], *twins]

    kv_turned = jnp.concatenate([w_key[0].T, w_value[0].T], axis=0)
    routes = []
    for source in range(N_TP):
        half, place = divmod(source, N_TP // 2)
        routes.append((source, (place ^ 1) * 2 + half))
    kv_turned = lax.ppermute(kv_turned, TP, routes)
    gain = norm_gain[0]
    gain_high = lax.reduce_precision(gain, 8, 7)
    gain_mid = lax.reduce_precision(gain - gain_high, 8, 7)
    gain_low = gain - gain_high - gain_mid
    gain_rows = jnp.stack([gain_high, gain_mid, gain_low]).astype(bf16)
    kv_turned = jnp.concatenate([kv_turned, jnp.pad(gain_rows, ((0, GAIN_ROWS - 3), (0, 0)))], axis=0)

    blocks_q = spread(
        lambda block: lax.dynamic_slice_in_dim(w_query[0], block * part, part, axis=0),
    )
    blocks_kv = spread(
        lambda block: lax.dynamic_slice_in_dim(kv_turned, block * part, part, axis=1),
    )
    local_ids = token_ids - section_index * vocab_rows
    inside = (local_ids >= 0) & (local_ids < vocab_rows)
    picked = jnp.take(embed_table, jnp.clip(local_ids, 0, vocab_rows - 1), axis=0)
    picked = jnp.where(inside[:, :, None], picked, jnp.zeros((), bf16))
    feats = embed_table.shape[1]
    sent = picked.reshape(micros, N_TP, own_rows, feats).transpose(1, 0, 2, 3)
    came = lax.all_to_all(sent, TP, 0, 0, tiled=True)
    came = came.reshape(N_Y, N_TP // N_Y, micros, own_rows, feats).transpose(0, 2, 3, 1, 4)
    found = lax.all_to_all(came.reshape(layers, own_rows, part), SECTION, 0, 0, tiled=True)
    resid = jnp.sum(found.astype(f32), axis=0).astype(bf16)

    blocks_out = spread(
        lambda block: lax.dynamic_slice_in_dim(w_out[0], block * part, part, axis=1), resid
    )

    seen_q, seen_k, seen_v, seen_out, _ = lax.optimization_barrier(
        (w_query[0], w_key[0], w_value[0], w_out[0], came)
    )
    weight_local = jnp.maximum(
        jnp.max(jnp.abs(seen_q), axis=1),
        jnp.maximum(jnp.max(jnp.abs(seen_k), axis=1), jnp.max(jnp.abs(seen_v), axis=1)),
    )
    out_peak = jnp.max(jnp.abs(seen_out), axis=1).astype(f32)

    cosine, sine = rope_tables(length, HEAD_DIM)
    cosine = jnp.concatenate([cosine, cosine], axis=1)
    sine = jnp.concatenate([-sine, sine], axis=1)
    tables = (cosine, sine, cosine.T, sine.T)
    state = jnp.stack([jnp.int32(0), y_index, core_index]).astype(jnp.int32)

    kv_at = heads_here * length
    stat_at = kv_at + 2 * kv_cols

    def one_layer(state, gathered, resid):
        packed = front(state, gathered, blocks_q, blocks_kv)
        packed = lax.all_to_all(packed, "y", 0, 0, tiled=True)
        summed = jnp.sum(packed.astype(f32), axis=0)
        mean = (summed[stat_at] + summed[stat_at + 8]) / width
        inverse = lax.rsqrt(mean + norm_eps)
        kv_rows = (summed[kv_at:stat_at] * inverse[None, :]).astype(bf16)
        kv_all = copy_for_each(kv_rows, HALF)
        head_part, peaks = back(
            state, gathered, summed, kv_all, tables, blocks_out, blocks_kv
        )
        shares = lax.all_to_all(head_part.reshape(N_TP, own_rows, part), TP, 0, 0, tiled=True)
        shares, peaks, state = lax.optimization_barrier((shares, peaks, state))
        state = state + (jnp.arange(3, dtype=jnp.int32) == 0)
        mixed = jnp.sum(shares.astype(f32), axis=0)
        return (resid.astype(f32) + mixed).astype(bf16), peaks, state

    rows = weight_local.reshape(-1, part)
    both = copy_for_each(jnp.concatenate([resid, rows], axis=0), TP)
    weight_peak = jnp.max(both[:, own_rows:], axis=0).reshape(width).astype(f32)
    resid, first_peaks, state = one_layer(state, both[:, :own_rows].reshape(length, part), resid)

    def advance(carry):
        layer, resid, stored, peaks, state = carry
        gathered = copy_for_each(resid, TP).reshape(length, part)
        resid, fresh, state = one_layer(state, gathered, resid)
        layer, resid = lax.optimization_barrier((layer, resid))
        stored = lax.dynamic_update_index_in_dim(stored, resid, layer, 0)
        peaks = lax.dynamic_update_slice_in_dim(peaks, fresh, layer, 0)
        return layer + 1, resid, stored, peaks, state

    stored = jnp.zeros((layers, own_rows, part), bf16).at[0].set(resid)
    peaks = jnp.zeros((layers, part + query_cols), f32).at[0].set(first_peaks[0])
    start = (jnp.uint32(1), resid, stored, peaks, state)
    _, _, stored, peaks, _ = lax.while_loop(lambda carry: carry[0] < layers, advance, start)

    peaks = lax.all_to_all(peaks.astype(bf16), SECTION, 0, 0, tiled=True).astype(f32)
    peaks = peaks.reshape(N_Y, N_CORE, part + query_cols).max(axis=1)
    act_peak = peaks[:, :part].reshape(width)
    head_peak = peaks[0, part:]
    kept = lax.all_to_all(stored, SECTION, 0, 0, tiled=True)
    kept = kept.reshape(N_Y, N_CORE, own_rows, part).transpose(1, 2, 0, 3)
    kept = kept.reshape(micros, own_rows, width)

    alpha_exp = alpha_num[0].astype(f32) / 10.0
    scale_in = smoothing(act_peak, weight_peak, alpha_exp)
    scale_out = smoothing(head_peak, out_peak, alpha_exp)
    smooth_query, smooth_key, smooth_value = (
        (w.astype(f32) * scale_in[None, :, None]).astype(bf16) for w in (w_query, w_key, w_value)
    )
    return (kept[None], scale_in[None], scale_out[None], smooth_query, smooth_key, smooth_value)


def solution(mesh):
    split = Mesh(mesh.devices.reshape(N_Y, N_CORE, 4, 2, 2), ("y", "core", "x", "zh", "zl"))
    return jax.shard_map(
        program,
        mesh=split,
        in_specs=(
            P(),
            P(),
            P(SECTION, TP),
            P(SECTION, None),
            P(SECTION, None, TP),
            P(SECTION, None, TP),
            P(SECTION, None, TP),
            P(SECTION, TP, None),
        ),
        out_specs=(
            P(SECTION, None, TP, None),
            P(SECTION, None),
            P(SECTION, TP),
            P(SECTION, None, TP),
            P(SECTION, None, TP),
            P(SECTION, None, TP),
        ),
        check_vma=False,
    )
```

```python
import math

import jax
import jax.numpy as jnp
from jax import lax
from jax.experimental import pallas as pl
from jax.experimental.pallas import tpu as pltpu
from jax.sharding import Mesh
from jax.sharding import PartitionSpec as P


HEAD_DIM = 128
TP = ("x", "zh", "zl")
HALF = ("x", "zh")
SECTION = ("y", "core")
N_Y = 4
N_CORE = 2
N_TP = 16
GAIN_ROWS = 16

norm_eps = 1e-05
stat_eps = 1e-05
rope_base = 500000.0


def copy_for_each(value, axis):
    count = lax.axis_size(axis)
    return lax.all_to_all(
        jnp.broadcast_to(value[None], (count, *value.shape)), axis, 0, 0, tiled=True
    )


def rope_tables(length, head_size):
    halves = head_size // 2
    freqs = jnp.exp(-math.log(rope_base) * 2.0 * jnp.arange(halves, dtype=jnp.float32) / head_size)
    angles = jnp.arange(length, dtype=jnp.float32)[:, None] * freqs[None, :]
    return (jnp.cos(angles), jnp.sin(angles))


def smoothing(act_peak, weight_peak, alpha_exp):
    return jnp.exp(
        alpha_exp * jnp.log(act_peak + stat_eps)
        - (1.0 - alpha_exp) * jnp.log(weight_peak + stat_eps)
    )


def fetch(choice, sources, target, sem):
    for number, source in enumerate(sources):

        @pl.when(choice == number)
        def _():
            pltpu.make_async_copy(source, target, sem).start()


def choice_of(state_ref):
    layer = state_ref[0]
    step = (state_ref[1] - layer // N_CORE + N_Y) % N_Y
    return jnp.where(layer % N_CORE == state_ref[2], step, step + N_Y)


def front_body(state_ref, x_ref, *refs):
    count = 2 * N_Y
    q_refs, kv_refs = refs[:count], refs[count : 2 * count]
    out_ref, q_buf, kv_buf, sems = refs[2 * count :]
    choice = choice_of(state_ref)
    fetch(choice, kv_refs, kv_buf, sems.at[0])
    fetch(choice, q_refs, q_buf, sems.at[1])
    values = x_ref[...].astype(jnp.float32)
    length, _ = values.shape
    square = jnp.sum(values * values, axis=1, keepdims=True)
    square = jnp.broadcast_to(square, (length, HEAD_DIM)).T[:8]
    high = square.astype(jnp.bfloat16)
    low = (square - high.astype(jnp.float32)).astype(jnp.bfloat16)
    pltpu.make_async_copy(kv_refs[0], kv_buf, sems.at[0]).wait()
    rows = kv_buf.shape[0] - GAIN_ROWS
    gain = kv_buf[rows:, :].astype(jnp.float32)
    gain = jnp.sum(gain, axis=0, keepdims=True)
    lhs = (values * gain).astype(jnp.bfloat16)
    kv_part = lax.dot_general(
        kv_buf[:rows, :], lhs, (((1,), (1,)), ((), ())), preferred_element_type=jnp.float32
    ).astype(jnp.bfloat16)
    pltpu.make_async_copy(q_refs[0], q_buf, sems.at[1]).wait()
    query = jnp.dot(lhs, q_buf[...], preferred_element_type=jnp.float32).astype(jnp.bfloat16)
    heads = query.shape[1] // HEAD_DIM
    for copy in range(N_Y):
        for h in range(heads):
            out_ref[copy, h * length : (h + 1) * length, :] = query[
                :, h * HEAD_DIM : (h + 1) * HEAD_DIM
            ]
        at = heads * length
        out_ref[copy, at : at + rows, :] = kv_part
        out_ref[copy, at + rows : at + rows + 8, :] = high
        out_ref[copy, at + rows + 8 :, :] = low


def back_body(
    state_ref, x_ref, sums_ref, kv_ref, cos_ref, sin_ref, cos_t_ref, sin_t_ref, *refs
):
    f32, bf16 = jnp.float32, jnp.bfloat16
    count = 2 * N_Y
    w_refs, g_refs = refs[:count], refs[count : 2 * count]
    out_ref, peaks_ref, w_buf, g_buf, sems = refs[2 * count :]
    choice = choice_of(state_ref)
    first_gain = g_refs[0].shape[0] - GAIN_ROWS
    g_refs = [ref.at[pl.ds(first_gain, GAIN_ROWS), :] for ref in g_refs]
    fetch(choice, g_refs, g_buf, sems.at[0])
    fetch(choice, w_refs, w_buf, sems.at[1])
    length, part = x_ref.shape
    query_cols = w_buf.shape[0]
    heads = query_cols // HEAD_DIM
    pieces = kv_ref.shape[0] // heads
    kv_cols = kv_ref.shape[1] // 2
    stat_at = heads * length + 2 * kv_cols
    square = sums_ref[stat_at : stat_at + 1, :] + sums_ref[stat_at + 8 : stat_at + 9, :]
    inverse = lax.rsqrt(square / (part * N_Y) + norm_eps)
    inverse = jnp.broadcast_to(inverse, (HEAD_DIM, length)).T
    rows = lax.broadcasted_iota(jnp.int32, (length, length), 0)
    cols = lax.broadcasted_iota(jnp.int32, (length, length), 1)
    halves = HEAD_DIM // 2
    outs = []
    for h in range(heads):
        of_head = [kv_ref[h * pieces + (piece ^ 1)] for piece in range(pieces)]
        key_t = jnp.concatenate([piece[:kv_cols] for piece in of_head], axis=0).astype(f32)
        value_t = jnp.concatenate([piece[kv_cols:] for piece in of_head], axis=0)
        turned = jnp.concatenate([key_t[halves:], key_t[:halves]], axis=0)
        key_rot = (key_t * cos_t_ref[...] + turned * sin_t_ref[...]).astype(bf16)
        query = sums_ref[h * length : (h + 1) * length, :] * inverse
        query_rot = query * cos_ref[...] + pltpu.roll(query, halves, 1) * sin_ref[...]
        scores = jnp.dot(query_rot.astype(bf16), key_rot, preferred_element_type=f32)
        scores = jnp.where(rows >= cols, scores / math.sqrt(HEAD_DIM), -1e30)
        scores = jnp.exp(scores - jnp.max(scores, axis=1, keepdims=True))
        probs = (scores / jnp.sum(scores, axis=1, keepdims=True)).astype(bf16)
        outs.append(
            lax.dot_general(
                probs, value_t, (((1,), (1,)), ((), ())), preferred_element_type=f32
            ).astype(bf16)
        )
    attended = jnp.concatenate(outs, axis=1)
    peaks_ref[:, part:] = jnp.max(jnp.abs(attended.astype(f32)), axis=0, keepdims=True)
    pltpu.make_async_copy(g_refs[0], g_buf, sems.at[0]).wait()
    for at in range(0, part, HEAD_DIM):
        block = x_ref[:, at : at + HEAD_DIM].astype(f32)
        gain = g_buf[:, at : at + HEAD_DIM].astype(f32)
        gain = jnp.sum(gain, axis=0, keepdims=True)
        normed = (block * inverse * gain).astype(bf16).astype(f32)
        peaks_ref[:, at : at + HEAD_DIM] = jnp.max(jnp.abs(normed), axis=0, keepdims=True)
    pltpu.make_async_copy(w_refs[0], w_buf, sems.at[1]).wait()
    out_ref[...] = jnp.dot(attended, w_buf[...], preferred_element_type=f32).astype(bf16)


def front(state, gathered, blocks_q, blocks_kv):
    length = gathered.shape[0]
    rows = blocks_q[0].shape[1] + blocks_kv[0].shape[0]
    hbm = pl.BlockSpec(memory_space=pl.ANY)
    vmem = pl.BlockSpec(memory_space=pltpu.VMEM)
    return pl.pallas_call(
        front_body,
        out_shape=jax.ShapeDtypeStruct((N_Y, rows, length), jnp.bfloat16),
        in_specs=[pl.BlockSpec(memory_space=pltpu.SMEM), vmem, *[hbm] * (4 * N_Y)],
        out_specs=vmem,
        scratch_shapes=[
            pltpu.VMEM(blocks_q[0].shape, jnp.bfloat16),
            pltpu.VMEM(blocks_kv[0].shape, jnp.bfloat16),
            pltpu.SemaphoreType.DMA((2,)),
        ],
        compiler_params=pltpu.CompilerParams(vmem_limit_bytes=16 << 20),
        name="front",
    )(state, gathered, *blocks_q, *blocks_kv)


def back(state, gathered, sums, kv_all, tables, blocks, blocks_kv):
    length, part = gathered.shape
    hbm = pl.BlockSpec(memory_space=pl.ANY)
    vmem = pl.BlockSpec(memory_space=pltpu.VMEM)
    return pl.pallas_call(
        back_body,
        out_shape=(
            jax.ShapeDtypeStruct((length, part), jnp.bfloat16),
            jax.ShapeDtypeStruct((1, part + blocks[0].shape[0]), jnp.float32),
        ),
        in_specs=[
            pl.BlockSpec(memory_space=pltpu.SMEM),
            *[vmem] * 7,
            *[hbm] * (4 * N_Y),
        ],
        out_specs=(vmem, vmem),
        scratch_shapes=[
            pltpu.VMEM(blocks[0].shape, jnp.bfloat16),
            pltpu.VMEM((GAIN_ROWS, part), jnp.bfloat16),
            pltpu.SemaphoreType.DMA((2,)),
        ],
        compiler_params=pltpu.CompilerParams(vmem_limit_bytes=16 << 20),
        name="back",
    )(state, gathered, sums, kv_all, *tables, *blocks, *blocks_kv)


def program(token_ids, alpha_num, embed_table, norm_gain, w_query, w_key, w_value, w_out):
    bf16, f32 = jnp.bfloat16, jnp.float32
    y_index = lax.axis_index("y")
    core_index = lax.axis_index("core")
    section_index = lax.axis_index(SECTION)
    micros, length = token_ids.shape
    vocab_rows = embed_table.shape[0]
    layers = N_Y * N_CORE
    own_rows = length // N_TP
    width = w_query.shape[1]
    part = width // N_Y
    query_cols = w_query.shape[2]
    kv_cols = w_key.shape[2]
    heads_here = query_cols // HEAD_DIM

    swap = [(0, 1), (1, 0)]

    def spread(block_for, after=None):
        own = {step: block_for((y_index + step) % N_Y) for step in (0, 1, 3, 2)}
        if after is not None:
            own, _ = lax.optimization_barrier((own, after))
        for step in (1, 3, 2):
            turn = [(i, (i + step) % N_Y) for i in range(N_Y)]
            own[step] = lax.ppermute(own[step], "y", turn)
        twins = []
        for step in range(N_Y):
            twins.append(lax.ppermute(own[step], "core", swap))
        return [*[own[step] for step in range(N_Y)], *twins]

    kv_turned = jnp.concatenate([w_key[0].T, w_value[0].T], axis=0)
    routes = []
    for source in range(N_TP):
        half, place = divmod(source, N_TP // 2)
        routes.append((source, (place ^ 1) * 2 + half))
    kv_turned = lax.ppermute(kv_turned, TP, routes)
    gain = norm_gain[0]
    gain_high = lax.reduce_precision(gain, 8, 7)
    gain_mid = lax.reduce_precision(gain - gain_high, 8, 7)
    gain_low = gain - gain_high - gain_mid
    gain_rows = jnp.stack([gain_high, gain_mid, gain_low]).astype(bf16)
    kv_turned = jnp.concatenate([kv_turned, jnp.pad(gain_rows, ((0, GAIN_ROWS - 3), (0, 0)))], axis=0)

    blocks_q = spread(
        lambda block: lax.dynamic_slice_in_dim(w_query[0], block * part, part, axis=0),
    )
    blocks_kv = spread(
        lambda block: lax.dynamic_slice_in_dim(kv_turned, block * part, part, axis=1),
    )
    local_ids = token_ids - section_index * vocab_rows
    inside = (local_ids >= 0) & (local_ids < vocab_rows)
    picked = jnp.take(embed_table, jnp.clip(local_ids, 0, vocab_rows - 1), axis=0)
    picked = jnp.where(inside[:, :, None], picked, jnp.zeros((), bf16))
    feats = embed_table.shape[1]
    sent = picked.reshape(micros, N_TP, own_rows, feats).transpose(1, 0, 2, 3)
    came = lax.all_to_all(sent, TP, 0, 0, tiled=True)
    came = came.reshape(N_Y, N_TP // N_Y, micros, own_rows, feats).transpose(0, 2, 3, 1, 4)
    found = lax.all_to_all(came.reshape(layers, own_rows, part), SECTION, 0, 0, tiled=True)
    resid = jnp.sum(found.astype(f32), axis=0).astype(bf16)

    blocks_out = spread(
        lambda block: lax.dynamic_slice_in_dim(w_out[0], block * part, part, axis=1), resid
    )

    seen_q, seen_k, seen_v, seen_out, _ = lax.optimization_barrier(
        (w_query[0], w_key[0], w_value[0], w_out[0], came)
    )
    weight_local = jnp.maximum(
        jnp.max(jnp.abs(seen_q), axis=1),
        jnp.maximum(jnp.max(jnp.abs(seen_k), axis=1), jnp.max(jnp.abs(seen_v), axis=1)),
    )
    out_peak = jnp.max(jnp.abs(seen_out), axis=1).astype(f32)

    cosine, sine = rope_tables(length, HEAD_DIM)
    cosine = jnp.concatenate([cosine, cosine], axis=1)
    sine = jnp.concatenate([-sine, sine], axis=1)
    tables = (cosine, sine, cosine.T, sine.T)
    state = jnp.stack([jnp.int32(0), y_index, core_index]).astype(jnp.int32)

    kv_at = heads_here * length
    stat_at = kv_at + 2 * kv_cols

    def one_layer(state, gathered, resid):
        packed = front(state, gathered, blocks_q, blocks_kv)
        packed = lax.all_to_all(packed, "y", 0, 0, tiled=True)
        summed = jnp.sum(packed.astype(f32), axis=0)
        mean = (summed[stat_at] + summed[stat_at + 8]) / width
        inverse = lax.rsqrt(mean + norm_eps)
        kv_rows = (summed[kv_at:stat_at] * inverse[None, :]).astype(bf16)
        kv_all = copy_for_each(kv_rows, HALF)
        head_part, peaks = back(
            state, gathered, summed, kv_all, tables, blocks_out, blocks_kv
        )
        shares = lax.all_to_all(head_part.reshape(N_TP, own_rows, part), TP, 0, 0, tiled=True)
        shares, peaks = lax.optimization_barrier((shares, peaks))
        mixed = jnp.sum(shares.astype(f32), axis=0)
        return (resid.astype(f32) + mixed).astype(bf16), peaks

    rows = weight_local.reshape(-1, part)
    both = copy_for_each(jnp.concatenate([resid, rows], axis=0), TP)
    weight_peak = jnp.max(both[:, own_rows:], axis=0).reshape(width).astype(f32)
    resid, first_peaks = one_layer(
        state, both[:, :own_rows].reshape(length, part), resid
    )

    def advance(carry):
        layer, resid, stored, peaks = carry
        now = state + layer.astype(jnp.int32) * (jnp.arange(3, dtype=jnp.int32) == 0)
        resid, now = lax.optimization_barrier((resid, now))
        gathered = copy_for_each(resid, TP).reshape(length, part)
        resid, fresh = one_layer(now, gathered, resid)
        layer, resid = lax.optimization_barrier((layer, resid))
        stored = lax.dynamic_update_index_in_dim(stored, resid, layer, 0)
        peaks = lax.dynamic_update_slice_in_dim(peaks, fresh, layer, 0)
        return layer + 1, resid, stored, peaks

    stored = jnp.zeros((layers, own_rows, part), bf16).at[0].set(resid)
    peaks = jnp.zeros((layers, part + query_cols), f32).at[0].set(first_peaks[0])
    start = (jnp.uint32(1), resid, stored, peaks)
    _, _, stored, peaks = lax.while_loop(lambda carry: carry[0] < layers, advance, start)

    peaks = lax.all_to_all(peaks.astype(bf16), SECTION, 0, 0, tiled=True).astype(f32)
    peaks = peaks.reshape(N_Y, N_CORE, part + query_cols).max(axis=1)
    act_peak = peaks[:, :part].reshape(width)
    head_peak = peaks[0, part:]
    kept = lax.all_to_all(stored, SECTION, 0, 0, tiled=True)
    kept = kept.reshape(N_Y, N_CORE, own_rows, part).transpose(1, 2, 0, 3)
    kept = kept.reshape(micros, own_rows, width)

    alpha_exp = alpha_num[0].astype(f32) / 10.0
    scale_in = smoothing(act_peak, weight_peak, alpha_exp)
    scale_out = smoothing(head_peak, out_peak, alpha_exp)
    smooth_query, smooth_key, smooth_value = (
        (w.astype(f32) * scale_in[None, :, None]).astype(bf16) for w in (w_query, w_key, w_value)
    )
    return (kept[None], scale_in[None], scale_out[None], smooth_query, smooth_key, smooth_value)


def solution(mesh):
    split = Mesh(mesh.devices.reshape(N_Y, N_CORE, 4, 2, 2), ("y", "core", "x", "zh", "zl"))
    return jax.shard_map(
        program,
        mesh=split,
        in_specs=(
            P(),
            P(),
            P(SECTION, TP),
            P(SECTION, None),
            P(SECTION, None, TP),
            P(SECTION, None, TP),
            P(SECTION, None, TP),
            P(SECTION, TP, None),
        ),
        out_specs=(
            P(SECTION, None, TP, None),
            P(SECTION, None),
            P(SECTION, TP),
            P(SECTION, None, TP),
            P(SECTION, None, TP),
            P(SECTION, None, TP),
        ),
        check_vma=False,
    )
```

```python
import math

import jax
import jax.numpy as jnp
from jax import lax
from jax.experimental import pallas as pl
from jax.experimental.pallas import tpu as pltpu
from jax.sharding import Mesh
from jax.sharding import PartitionSpec as P


HEAD_DIM = 128
TP = ("x", "zh", "zl")
HALF = ("x", "zh")
SECTION = ("y", "core")
N_Y = 4
N_CORE = 2
N_TP = 16
GAIN_ROWS = 16

norm_eps = 1e-05
stat_eps = 1e-05
rope_base = 500000.0


def copy_for_each(value, axis):
    count = lax.axis_size(axis)
    return lax.all_to_all(
        jnp.broadcast_to(value[None], (count, *value.shape)), axis, 0, 0, tiled=True
    )


def rope_tables(length, head_size):
    halves = head_size // 2
    freqs = jnp.exp(-math.log(rope_base) * 2.0 * jnp.arange(halves, dtype=jnp.float32) / head_size)
    angles = jnp.arange(length, dtype=jnp.float32)[:, None] * freqs[None, :]
    return (jnp.cos(angles), jnp.sin(angles))


def smoothing(act_peak, weight_peak, alpha_exp):
    return jnp.exp(
        alpha_exp * jnp.log(act_peak + stat_eps)
        - (1.0 - alpha_exp) * jnp.log(weight_peak + stat_eps)
    )


def fetch(choice, sources, target, sem):
    for number, source in enumerate(sources):

        @pl.when(choice == number)
        def _():
            pltpu.make_async_copy(source, target, sem).start()


def choice_of(state_ref):
    layer = state_ref[0]
    step = (state_ref[1] - layer // N_CORE + N_Y) % N_Y
    return jnp.where(layer % N_CORE == state_ref[2], step, step + N_Y)


def front_body(state_ref, x_ref, *refs):
    count = 2 * N_Y
    q_refs, kv_refs = refs[:count], refs[count : 2 * count]
    out_ref, q_buf, kv_buf, sems = refs[2 * count :]
    choice = choice_of(state_ref)
    fetch(choice, kv_refs, kv_buf, sems.at[0])
    half = q_buf.shape[0] // 2
    tops = [ref.at[pl.ds(0, half), :] for ref in q_refs]
    ends = [ref.at[pl.ds(half, half), :] for ref in q_refs]
    fetch(choice, tops, q_buf.at[pl.ds(0, half), :], sems.at[1])
    fetch(choice, ends, q_buf.at[pl.ds(half, half), :], sems.at[2])
    values = x_ref[...].astype(jnp.float32)
    length, _ = values.shape
    square = jnp.sum(values * values, axis=1, keepdims=True)
    square = jnp.broadcast_to(square, (length, HEAD_DIM)).T[:8]
    high = square.astype(jnp.bfloat16)
    low = (square - high.astype(jnp.float32)).astype(jnp.bfloat16)
    pltpu.make_async_copy(kv_refs[0], kv_buf, sems.at[0]).wait()
    rows = kv_buf.shape[0] - GAIN_ROWS
    gain = kv_buf[rows:, :].astype(jnp.float32)
    gain = jnp.sum(gain, axis=0, keepdims=True)
    lhs = (values * gain).astype(jnp.bfloat16)
    kv_part = lax.dot_general(
        kv_buf[:rows, :], lhs, (((1,), (1,)), ((), ())), preferred_element_type=jnp.float32
    ).astype(jnp.bfloat16)
    pltpu.make_async_copy(tops[0], q_buf.at[pl.ds(0, half), :], sems.at[1]).wait()
    query = jnp.dot(lhs[:, :half], q_buf[:half, :], preferred_element_type=jnp.float32)
    pltpu.make_async_copy(ends[0], q_buf.at[pl.ds(half, half), :], sems.at[2]).wait()
    query += jnp.dot(lhs[:, half:], q_buf[half:, :], preferred_element_type=jnp.float32)
    query = query.astype(jnp.bfloat16)
    heads = query.shape[1] // HEAD_DIM
    for copy in range(N_Y):
        for h in range(heads):
            out_ref[copy, h * length : (h + 1) * length, :] = query[
                :, h * HEAD_DIM : (h + 1) * HEAD_DIM
            ]
        at = heads * length
        out_ref[copy, at : at + rows, :] = kv_part
        out_ref[copy, at + rows : at + rows + 8, :] = high
        out_ref[copy, at + rows + 8 :, :] = low


def back_body(
    state_ref, x_ref, sums_ref, kv_ref, cos_ref, sin_ref, cos_t_ref, sin_t_ref, *refs
):
    f32, bf16 = jnp.float32, jnp.bfloat16
    count = 2 * N_Y
    w_refs, g_refs = refs[:count], refs[count : 2 * count]
    out_ref, peaks_ref, w_buf, g_buf, sems = refs[2 * count :]
    choice = choice_of(state_ref)
    first_gain = g_refs[0].shape[0] - GAIN_ROWS
    g_refs = [ref.at[pl.ds(first_gain, GAIN_ROWS), :] for ref in g_refs]
    fetch(choice, g_refs, g_buf, sems.at[0])
    fetch(choice, w_refs, w_buf, sems.at[1])
    length, part = x_ref.shape
    query_cols = w_buf.shape[0]
    heads = query_cols // HEAD_DIM
    pieces = kv_ref.shape[0] // heads
    kv_cols = kv_ref.shape[1] // 2
    stat_at = heads * length + 2 * kv_cols
    square = sums_ref[stat_at : stat_at + 1, :] + sums_ref[stat_at + 8 : stat_at + 9, :]
    inverse = lax.rsqrt(square / (part * N_Y) + norm_eps)
    inverse = jnp.broadcast_to(inverse, (HEAD_DIM, length)).T
    rows = lax.broadcasted_iota(jnp.int32, (length, length), 0)
    cols = lax.broadcasted_iota(jnp.int32, (length, length), 1)
    halves = HEAD_DIM // 2
    outs = []
    for h in range(heads):
        of_head = [kv_ref[h * pieces + (piece ^ 1)] for piece in range(pieces)]
        key_t = jnp.concatenate([piece[:kv_cols] for piece in of_head], axis=0).astype(f32)
        value_t = jnp.concatenate([piece[kv_cols:] for piece in of_head], axis=0)
        turned = jnp.concatenate([key_t[halves:], key_t[:halves]], axis=0)
        key_rot = (key_t * cos_t_ref[...] + turned * sin_t_ref[...]).astype(bf16)
        query = sums_ref[h * length : (h + 1) * length, :] * inverse
        query_rot = query * cos_ref[...] + pltpu.roll(query, halves, 1) * sin_ref[...]
        scores = jnp.dot(query_rot.astype(bf16), key_rot, preferred_element_type=f32)
        scores = jnp.where(rows >= cols, scores / math.sqrt(HEAD_DIM), -1e30)
        scores = jnp.exp(scores - jnp.max(scores, axis=1, keepdims=True))
        probs = (scores / jnp.sum(scores, axis=1, keepdims=True)).astype(bf16)
        outs.append(
            lax.dot_general(
                probs, value_t, (((1,), (1,)), ((), ())), preferred_element_type=f32
            ).astype(bf16)
        )
    attended = jnp.concatenate(outs, axis=1)
    peaks_ref[:, part:] = jnp.max(jnp.abs(attended.astype(f32)), axis=0, keepdims=True)
    pltpu.make_async_copy(g_refs[0], g_buf, sems.at[0]).wait()
    for at in range(0, part, HEAD_DIM):
        block = x_ref[:, at : at + HEAD_DIM].astype(f32)
        gain = g_buf[:, at : at + HEAD_DIM].astype(f32)
        gain = jnp.sum(gain, axis=0, keepdims=True)
        normed = (block * inverse * gain).astype(bf16).astype(f32)
        peaks_ref[:, at : at + HEAD_DIM] = jnp.max(jnp.abs(normed), axis=0, keepdims=True)
    pltpu.make_async_copy(w_refs[0], w_buf, sems.at[1]).wait()
    out_ref[...] = jnp.dot(attended, w_buf[...], preferred_element_type=f32).astype(bf16)


def front(state, gathered, blocks_q, blocks_kv):
    length = gathered.shape[0]
    rows = blocks_q[0].shape[1] + blocks_kv[0].shape[0]
    hbm = pl.BlockSpec(memory_space=pl.ANY)
    vmem = pl.BlockSpec(memory_space=pltpu.VMEM)
    return pl.pallas_call(
        front_body,
        out_shape=jax.ShapeDtypeStruct((N_Y, rows, length), jnp.bfloat16),
        in_specs=[pl.BlockSpec(memory_space=pltpu.SMEM), vmem, *[hbm] * (4 * N_Y)],
        out_specs=vmem,
        scratch_shapes=[
            pltpu.VMEM(blocks_q[0].shape, jnp.bfloat16),
            pltpu.VMEM(blocks_kv[0].shape, jnp.bfloat16),
            pltpu.SemaphoreType.DMA((3,)),
        ],
        compiler_params=pltpu.CompilerParams(vmem_limit_bytes=16 << 20),
        name="front",
    )(state, gathered, *blocks_q, *blocks_kv)


def back(state, gathered, sums, kv_all, tables, blocks, blocks_kv):
    length, part = gathered.shape
    hbm = pl.BlockSpec(memory_space=pl.ANY)
    vmem = pl.BlockSpec(memory_space=pltpu.VMEM)
    return pl.pallas_call(
        back_body,
        out_shape=(
            jax.ShapeDtypeStruct((length, part), jnp.bfloat16),
            jax.ShapeDtypeStruct((1, part + blocks[0].shape[0]), jnp.float32),
        ),
        in_specs=[
            pl.BlockSpec(memory_space=pltpu.SMEM),
            *[vmem] * 7,
            *[hbm] * (4 * N_Y),
        ],
        out_specs=(vmem, vmem),
        scratch_shapes=[
            pltpu.VMEM(blocks[0].shape, jnp.bfloat16),
            pltpu.VMEM((GAIN_ROWS, part), jnp.bfloat16),
            pltpu.SemaphoreType.DMA((2,)),
        ],
        compiler_params=pltpu.CompilerParams(vmem_limit_bytes=16 << 20),
        name="back",
    )(state, gathered, sums, kv_all, *tables, *blocks, *blocks_kv)


def program(token_ids, alpha_num, embed_table, norm_gain, w_query, w_key, w_value, w_out):
    bf16, f32 = jnp.bfloat16, jnp.float32
    y_index = lax.axis_index("y")
    core_index = lax.axis_index("core")
    section_index = lax.axis_index(SECTION)
    micros, length = token_ids.shape
    vocab_rows = embed_table.shape[0]
    layers = N_Y * N_CORE
    own_rows = length // N_TP
    width = w_query.shape[1]
    part = width // N_Y
    query_cols = w_query.shape[2]
    kv_cols = w_key.shape[2]
    heads_here = query_cols // HEAD_DIM

    swap = [(0, 1), (1, 0)]

    def spread(block_for, after=None):
        own = {step: block_for((y_index + step) % N_Y) for step in (0, 1, 3, 2)}
        if after is not None:
            own, _ = lax.optimization_barrier((own, after))
        for step in (1, 3, 2):
            turn = [(i, (i + step) % N_Y) for i in range(N_Y)]
            own[step] = lax.ppermute(own[step], "y", turn)
        twins = []
        for step in range(N_Y):
            twins.append(lax.ppermute(own[step], "core", swap))
        return [*[own[step] for step in range(N_Y)], *twins]

    kv_turned = jnp.concatenate([w_key[0].T, w_value[0].T], axis=0)
    routes = []
    for source in range(N_TP):
        half, place = divmod(source, N_TP // 2)
        routes.append((source, (place ^ 1) * 2 + half))
    kv_turned = lax.ppermute(kv_turned, TP, routes)
    gain = norm_gain[0]
    gain_high = lax.reduce_precision(gain, 8, 7)
    gain_mid = lax.reduce_precision(gain - gain_high, 8, 7)
    gain_low = gain - gain_high - gain_mid
    gain_rows = jnp.stack([gain_high, gain_mid, gain_low]).astype(bf16)
    kv_turned = jnp.concatenate([kv_turned, jnp.pad(gain_rows, ((0, GAIN_ROWS - 3), (0, 0)))], axis=0)

    blocks_q = spread(
        lambda block: lax.dynamic_slice_in_dim(w_query[0], block * part, part, axis=0),
    )
    blocks_kv = spread(
        lambda block: lax.dynamic_slice_in_dim(kv_turned, block * part, part, axis=1),
    )
    local_ids = token_ids - section_index * vocab_rows
    inside = (local_ids >= 0) & (local_ids < vocab_rows)
    picked = jnp.take(embed_table, jnp.clip(local_ids, 0, vocab_rows - 1), axis=0)
    picked = jnp.where(inside[:, :, None], picked, jnp.zeros((), bf16))
    feats = embed_table.shape[1]
    sent = picked.reshape(micros, N_TP, own_rows, feats).transpose(1, 0, 2, 3)
    came = lax.all_to_all(sent, TP, 0, 0, tiled=True)
    came = came.reshape(N_Y, N_TP // N_Y, micros, own_rows, feats).transpose(0, 2, 3, 1, 4)
    found = lax.all_to_all(came.reshape(layers, own_rows, part), SECTION, 0, 0, tiled=True)
    resid = jnp.sum(found.astype(f32), axis=0).astype(bf16)

    blocks_out = spread(
        lambda block: lax.dynamic_slice_in_dim(w_out[0], block * part, part, axis=1),
    )

    seen_q, seen_k, seen_v, seen_out, _ = lax.optimization_barrier(
        (w_query[0], w_key[0], w_value[0], w_out[0], came)
    )
    weight_local = jnp.maximum(
        jnp.max(jnp.abs(seen_q), axis=1),
        jnp.maximum(jnp.max(jnp.abs(seen_k), axis=1), jnp.max(jnp.abs(seen_v), axis=1)),
    )
    out_peak = jnp.max(jnp.abs(seen_out), axis=1).astype(f32)

    cosine, sine = rope_tables(length, HEAD_DIM)
    cosine = jnp.concatenate([cosine, cosine], axis=1)
    sine = jnp.concatenate([-sine, sine], axis=1)
    tables = (cosine, sine, cosine.T, sine.T)
    state = jnp.stack([jnp.int32(0), y_index, core_index]).astype(jnp.int32)

    kv_at = heads_here * length
    stat_at = kv_at + 2 * kv_cols

    def one_layer(state, gathered, resid):
        packed = front(state, gathered, blocks_q, blocks_kv)
        packed = lax.all_to_all(packed, "y", 0, 0, tiled=True)
        summed = jnp.sum(packed.astype(f32), axis=0)
        mean = (summed[stat_at] + summed[stat_at + 8]) / width
        inverse = lax.rsqrt(mean + norm_eps)
        kv_rows = (summed[kv_at:stat_at] * inverse[None, :]).astype(bf16)
        kv_all = copy_for_each(kv_rows, HALF)
        head_part, peaks = back(
            state, gathered, summed, kv_all, tables, blocks_out, blocks_kv
        )
        shares = lax.all_to_all(head_part.reshape(N_TP, own_rows, part), TP, 0, 0, tiled=True)
        shares, peaks = lax.optimization_barrier((shares, peaks))
        mixed = jnp.sum(shares.astype(f32), axis=0)
        return (resid.astype(f32) + mixed).astype(bf16), peaks

    rows = weight_local.reshape(-1, part)
    both = copy_for_each(jnp.concatenate([resid, rows], axis=0), TP)
    weight_peak = jnp.max(both[:, own_rows:], axis=0).reshape(width).astype(f32)
    resid, first_peaks = one_layer(
        state, both[:, :own_rows].reshape(length, part), resid
    )

    def advance(carry):
        layer, resid, stored, peaks = carry
        now = state + layer.astype(jnp.int32) * (jnp.arange(3, dtype=jnp.int32) == 0)
        resid, now = lax.optimization_barrier((resid, now))
        gathered = copy_for_each(resid, TP).reshape(length, part)
        resid, fresh = one_layer(now, gathered, resid)
        layer, resid = lax.optimization_barrier((layer, resid))
        stored = lax.dynamic_update_index_in_dim(stored, resid, layer, 0)
        peaks = lax.dynamic_update_slice_in_dim(peaks, fresh, layer, 0)
        return layer + 1, resid, stored, peaks

    stored = jnp.zeros((layers, own_rows, part), bf16).at[0].set(resid)
    peaks = jnp.zeros((layers, part + query_cols), f32).at[0].set(first_peaks[0])
    start = (jnp.uint32(1), resid, stored, peaks)
    _, _, stored, peaks = lax.while_loop(lambda carry: carry[0] < layers, advance, start)

    peaks = lax.all_to_all(peaks.astype(bf16), SECTION, 0, 0, tiled=True).astype(f32)
    peaks = peaks.reshape(N_Y, N_CORE, part + query_cols).max(axis=1)
    act_peak = peaks[:, :part].reshape(width)
    head_peak = peaks[0, part:]
    kept = lax.all_to_all(stored, SECTION, 0, 0, tiled=True)
    kept = kept.reshape(N_Y, N_CORE, own_rows, part).transpose(1, 2, 0, 3)
    kept = kept.reshape(micros, own_rows, width)

    alpha_exp = alpha_num[0].astype(f32) / 10.0
    scale_in = smoothing(act_peak, weight_peak, alpha_exp)
    scale_out = smoothing(head_peak, out_peak, alpha_exp)
    smooth_query, smooth_key, smooth_value = (
        (w.astype(f32) * scale_in[None, :, None]).astype(bf16) for w in (w_query, w_key, w_value)
    )
    return (kept[None], scale_in[None], scale_out[None], smooth_query, smooth_key, smooth_value)


def solution(mesh):
    split = Mesh(mesh.devices.reshape(N_Y, N_CORE, 4, 2, 2), ("y", "core", "x", "zh", "zl"))
    return jax.shard_map(
        program,
        mesh=split,
        in_specs=(
            P(),
            P(),
            P(SECTION, TP),
            P(SECTION, None),
            P(SECTION, None, TP),
            P(SECTION, None, TP),
            P(SECTION, None, TP),
            P(SECTION, TP, None),
        ),
        out_specs=(
            P(SECTION, None, TP, None),
            P(SECTION, None),
            P(SECTION, TP),
            P(SECTION, None, TP),
            P(SECTION, None, TP),
            P(SECTION, None, TP),
        ),
        check_vma=False,
    )
```
